32 devices in a mesh: arcs: 8 (over y, x, core), tiles: 4 (over z).
Axes of the slice: x: 2, y: 2, z: 4, core: 2. Of those that a mesh axis runs over, the one named last changes fastest.
Arguments:
- design: bfloat16 [12288, 8192], P('arcs', 'tiles'), may hold values from -0.09375 to 0.09375
- observations: float32 [12288], P('arcs'), may hold values from -25 to 25
- solution: float32 [8192], P('tiles'), may hold values from -6 to 6
- arc_ids: int32 [8, 1536], P('arcs'), may hold values from 0 to 3, never falling along the last dimension, each value on 1 to 768 neighbouring positions
- block_live: int32 [8, 12], P('arcs'), may hold values 0 or 1
Outputs:
- normal: float32 [8192, 8192], P('arcs', 'tiles')
- rhs: float32 [8192], P('tiles')
The draws below stay inside these ranges and needn't reach their ends.
Inputs may be any that keep to these rules, and one draw needn't show every extreme that they name: `arc_ids`: the arcs of a group's rows never fall along its rows; an arc holds at most 768 rows and some arc exactly that many.
All inputs are finite; a program needn't handle non-finite values. No bound on the sum of `block_live` on one device may be relied on, other than what follows from the above.
Results may differ from the reference program's by a relative error of at most 0.0018.
Values may be sent and summed in bfloat16 or wider, within the bound.
A program may use at most 192 MiB of HBM per device.

```python
import math
import jax
import jax.numpy as jnp
import numpy as np
from jax import lax

COEF = 8192
ROWS_DEV = 1536
ARCS_DEV = 4
SEG_MOST = 768
BLOCKS = 12
TOTAL_ROWS = 12288
N_ARCS = 8


def draw_observations(key, part):
    first_key, second_key = jax.random.split(jax.random.fold_in(key, 11))
    position = jnp.arange(TOTAL_ROWS, dtype=jnp.int32)
    denominator = max(TOTAL_ROWS // ROWS_DEV - 1, 1)
    device_frac = (position // ROWS_DEV).astype(jnp.float32) / denominator
    group_scale = jnp.exp(jax.random.uniform(second_key, (TOTAL_ROWS // 64,), minval=-0.5, maxval=0.5))
    local_scale = jnp.repeat(group_scale, 64)
    noise = jnp.clip(jax.random.normal(first_key, (TOTAL_ROWS,)), -5.0, 5.0)
    return (noise * (1.0 + 2.0 * device_frac) * local_scale).astype(jnp.float32)


def set_ends(result, stream_key, low, high):
    index_at = [jax.random.randint(jax.random.fold_in(stream_key, axis), (), 0, length) for axis, length in enumerate(result.shape)]
    longest = result.shape.index(max(result.shape))
    neighbour = index_at[:longest] + [(index_at[longest] + 1) % result.shape[longest]] + index_at[longest + 1:]
    return result.at[tuple(index_at)].set(low).at[tuple(neighbour)].set(high)


def raised(drawn, stream_key, source, target, parts, factor):
    owner, partner = [(jnp.arange(drawn.shape[dim]) // (drawn.shape[dim] // parts)).reshape([-1 if axis == dim else 1 for axis in range(drawn.ndim)]) for dim in (source, target)]
    chosen = jax.random.permutation(stream_key, parts)[partner]
    strong = (owner == chosen) | (owner == (partner + parts // 2) % parts)
    return jnp.where(strong, factor * drawn, drawn)


def shard_levels(own_key, dims, cuts, low, largest):
    def one(dim, blocks):
        steps = jax.random.uniform(jax.random.fold_in(jax.random.fold_in(own_key, 6), dim), (blocks,), jnp.float32, low / len(cuts), largest / len(cuts))
        return jnp.repeat(jnp.exp(steps), dims[dim] // blocks).reshape((-1,) + (1,) * (len(dims) - dim - 1))

    level = one(*cuts[0])
    for cut in cuts[1:]:
        level = level * one(*cut)
    return level


def split_up(number_of, total, bound, skew):
    portions = [(1 << 20) // math.isqrt(standing ** skew) + 1 for standing in range(2, number_of + 1)]
    spare, holding = total - bound - (number_of - 1), [1] * (number_of - 1)
    while spare > 0:
        free = [i for i in range(number_of - 1) if holding[i] < bound]
        whole, budget = sum([portions[i] for i in free]), spare
        for i in free:
            more = min(bound - holding[i], max(1, budget * portions[i] // whole), spare)
            holding[i] = holding[i] + more
            spare = spare - more
    return np.array([bound] + holding)


def uneven(own_key, amount, total, most, skew):
    if amount == 2:
        one = jax.random.randint(own_key, (), max(1, total - most), min(most, total - 1) + 1)
        return jnp.stack([one, total - one])
    tallies = jnp.asarray(split_up(amount, total, most, skew), jnp.int32)
    twos = (amount - 1) // 2
    giver, receiver = tallies[1:1 + 2 * twos:2], tallies[2:2 + 2 * twos:2]
    margin = jnp.minimum(giver - 1, most - receiver)
    moved = jax.random.randint(jax.random.fold_in(own_key, 1), (twos,), 0, 1 << 20) % (margin + 1)
    tallies = tallies.at[1:1 + 2 * twos:2].set(giver - moved).at[2:2 + 2 * twos:2].set(receiver + moved)
    return tallies[jax.random.permutation(jax.random.fold_in(own_key, 2), amount)]


def gaussian(rng, shape, width, reach, cuts=(), kind=jnp.bfloat16):
    values = jax.random.normal(rng, shape, jnp.float32) * width
    if len(cuts) > 0:
        values = shard_levels(rng, shape, cuts, -0.22, 0.18) * values
    return jnp.clip(values, min=-reach, max=reach).astype(kind)


def gaussian_with(own_key, shape, width, limit, pieces, heavy, kind=jnp.bfloat16):
    entries = width * jax.random.normal(own_key, shape, jnp.float32)
    if pieces:
        entries = entries * shard_levels(own_key, shape, pieces, -0.22, 0.18)
    return jnp.clip(raised(entries, jax.random.fold_in(own_key, 3), *heavy), -limit, limit).astype(kind)


def setup_inputs(seed: int = 0) -> dict:
    key_of = jax.random.split(jax.random.key(seed), 6)
    design = gaussian_with(key_of[0], (TOTAL_ROWS, COEF), COEF ** -0.5, 0.09375, ((0, 8), (1, 4)), (0, 1, 8, 2.0))
    observations = draw_observations(jax.random.fold_in(key_of[5], 71), 0)
    solution = gaussian(key_of[2], (COEF,), 1.0, 6.0, ((0, 4),), jnp.float32)
    arc_ids = jax.vmap(lambda own: jnp.searchsorted(jnp.cumsum(uneven(own, ARCS_DEV, ROWS_DEV, SEG_MOST, 2)), jnp.arange(ROWS_DEV), side="right"))(jax.random.split(key_of[3], N_ARCS)).reshape((N_ARCS, ROWS_DEV)).astype(jnp.int32)
    block_live = set_ends((jax.random.randint(key_of[4], (N_ARCS, BLOCKS), 0, 4) < 3).astype(jnp.int32), jax.random.fold_in(key_of[4], 1), 0, 1)
    return {"design": design, "observations": observations, "solution": solution, "arc_ids": arc_ids, "block_live": block_live}


prior_rows = 4.0


def reference(design, observations, solution, arc_ids, block_live):
    groups = arc_ids.shape[0]
    per_group = arc_ids.shape[1]
    row_count = groups * per_group
    live_row = jnp.broadcast_to(block_live[:, :, None], (groups, block_live.shape[1], 128)).reshape(row_count).astype(jnp.float32)
    design_wide = design.astype(jnp.float32)
    predicted = jnp.dot(design_wide, solution, precision=lax.Precision.HIGHEST)
    residual = observations - predicted
    squares = (live_row * residual * residual).reshape(groups, per_group)
    live_group = live_row.reshape(groups, per_group)
    arc_match = (arc_ids[:, None, :] == jnp.arange(ARCS_DEV, dtype=jnp.int32)[None, :, None]).astype(jnp.float32)
    arc_squares = jnp.sum(arc_match * squares[:, None, :], axis=2)
    arc_counts = jnp.sum(arc_match * live_group[:, None, :], axis=2)
    variance_all = (jnp.sum(arc_squares) + 1.0) / (jnp.sum(arc_counts) + 1.0)
    arc_weight = variance_all / ((arc_squares + prior_rows * variance_all) / (arc_counts + prior_rows))
    row_weight = live_row * jnp.sum(arc_match * arc_weight[:, :, None], axis=1).reshape(row_count)
    weighted = (row_weight[:, None] * design_wide).astype(jnp.bfloat16)
    normal = jnp.dot(design_wide.T, weighted.astype(jnp.float32), precision=lax.Precision.HIGHEST)
    rhs = jnp.dot(design_wide.T, row_weight * residual, precision=lax.Precision.HIGHEST)
    return normal, rhs
```

```python
import functools

import jax
import jax.numpy as jnp
from jax import lax
from jax.experimental import pallas as pl
from jax.experimental.pallas import tpu as pltpu
from jax.sharding import PartitionSpec as P

ARCS_DEV = 4
STEP_ROWS = 256
LAG_JOIN = 1
LAG_OUT = 3
SLOTS = 4
MESH = pl.DeviceIdType.MESH

prior_rows = 4.0


def contract_rows(left, right):
    return lax.dot_general(
        left, right, (((0,), (0,)), ((), ())), preferred_element_type=jnp.float32
    )


def row_weights(design, observations, solution, arc_ids, block_live):
    row_count = design.shape[0]
    partial_value = jnp.dot(design.astype(jnp.float32), solution, precision=lax.Precision.HIGHEST)
    predicted = lax.psum(partial_value, "tiles")
    residual = observations - predicted
    live_row = (
        jnp.broadcast_to(block_live[0][:, None], (block_live.shape[1], 128))
        .reshape(row_count)
        .astype(jnp.float32)
    )
    arc_match = (arc_ids[0][None, :] == jnp.arange(ARCS_DEV, dtype=jnp.int32)[:, None]).astype(
        jnp.float32
    )
    squares = live_row * residual * residual
    arc_squares = jnp.sum(arc_match * squares[None, :], axis=1)
    arc_counts = jnp.sum(arc_match * live_row[None, :], axis=1)
    totals = lax.psum(jnp.stack([jnp.sum(arc_squares), jnp.sum(arc_counts)]), "arcs")
    variance_all = (totals[0] + 1.0) / (totals[1] + 1.0)
    arc_weight = variance_all / (
        (arc_squares + prior_rows * variance_all) / (arc_counts + prior_rows)
    )
    row_weight = live_row * jnp.sum(arc_match * arc_weight[:, None], axis=0)
    return row_weight, residual


def right_side(design, row_weight, residual):
    return lax.dot_general(
        design.astype(jnp.float32),
        row_weight * residual,
        (((0,), (0,)), ((), ())),
        precision=lax.Precision.HIGHEST,
    )


def general(design, observations, solution, arc_ids, block_live):
    design_all = lax.all_gather(design, "tiles", axis=1, tiled=True)
    row_weight, residual = row_weights(design, observations, solution, arc_ids, block_live)
    rhs = lax.psum(right_side(design, row_weight, residual), "arcs")
    weighted = (row_weight[:, None] * design).astype(jnp.bfloat16)
    normal = lax.psum_scatter(
        contract_rows(design_all, weighted), "arcs", scatter_dimension=0, tiled=True
    )
    return (normal, rhs)


def line_kernel(
    both_ref, weight_ref,
    out_ref, held_ref, twin_ref, sums_ref, last_sums_ref,
    right, left, partial, sent, joined, far_in, near_in, last_in, outer_in,
    load_sem, store_sem, a_send, w_send, b_send, twin_send, held_recv, twin_recv,
    stage_send, join_send, far_recv, near_recv, last_recv, outer_recv,
    sums_send, sums_recv, relay_send, relay_recv,
):
    n_cols, n_rows = both_ref.shape
    half = n_cols // 2
    chunk = STEP_ROWS
    n_chunks = half // chunk
    me, z = lax.axis_index("arcs"), lax.axis_index("tiles")
    core, chip = lax.rem(me, 2), lax.div(me, 2)
    x, y = lax.rem(chip, 2), lax.div(chip, 2)
    x_peer = me + 2 - 4 * x
    y_peer = me + 4 - 8 * y
    core_peer = me + 1 - 2 * core
    side = lax.div(z, 2)
    step_z = 1 - 2 * side
    inner = (z == 1) | (z == 2)
    outer = jnp.logical_not(inner)
    toward_z = z + step_z
    away_z = jnp.where(inner, z - step_z, z)

    def flip(a, b):
        return a + b - 2 * a * b

    def rows_of(h):
        return pl.ds(pl.multiple_of(h * chunk, chunk), chunk)

    def own_rows(h):
        return pl.ds(pl.multiple_of(core * half + h * chunk, chunk), chunk)

    def remote(src, dst, send, recv, a, zz):
        return pltpu.make_async_remote_copy(
            src_ref=src, dst_ref=dst, send_sem=send, recv_sem=recv,
            device_id=(a, zz), device_id_type=MESH,
        )

    def send_toward(h):
        slot = jnp.where(inner, 0, 1)
        return remote(both_ref.at[own_rows(h)], held_ref.at[slot, rows_of(h)],
                      a_send.at[h], held_recv.at[slot, h], me, toward_z)

    def send_away(h):
        return remote(both_ref.at[own_rows(h)], held_ref.at[0, rows_of(h)],
                      w_send.at[h], held_recv.at[0, h], me, away_z)

    def send_on(h):
        return remote(held_ref.at[1, rows_of(h)], held_ref.at[2, rows_of(h)],
                      b_send.at[h], held_recv.at[2, h], me, toward_z)

    def send_twin(h):
        return remote(held_ref.at[1, rows_of(h)], twin_ref.at[rows_of(h)],
                      twin_send.at[h], twin_recv.at[h], core_peer, z)

    def arrived(slot, h):
        return remote(held_ref.at[slot, rows_of(h)], held_ref.at[slot, rows_of(h)],
                      a_send.at[h], held_recv.at[slot, h], me, toward_z)

    barrier = pltpu.get_barrier_semaphore()
    for a, zz in ((x_peer, z), (y_peer, z), (core_peer, z), (me, toward_z)):
        pl.semaphore_signal(barrier, inc=1, device_id=(a, zz), device_id_type=MESH)

    @pl.when(inner)
    def _():
        pl.semaphore_signal(barrier, inc=1, device_id=(me, away_z), device_id_type=MESH)
        pl.semaphore_wait(barrier, 5)

    @pl.when(outer)
    def _():
        pl.semaphore_wait(barrier, 4)

    for h in range(n_chunks):
        send_toward(h).start()

        @pl.when(inner)
        def _():
            send_away(h).start()

    def load(src, dst):
        copy = pltpu.make_async_copy(src, dst, load_sem)
        copy.start()
        copy.wait()

    def weigh_into(kind, first, src):
        load(src, left)

        def body(i, carry):
            rows = pl.ds(pl.multiple_of(i * 32, 32), 32)
            value = left[rows, :].astype(jnp.float32) * weight_ref[...]
            at = pl.ds(pl.multiple_of(first + i * 32, 32), 32)
            right[kind, at, :] = value.astype(jnp.bfloat16)
            return carry

        lax.fori_loop(0, chunk // 32, body, 0)

    def prepare_own(i, carry):
        weigh_into(0, i * chunk, both_ref.at[rows_of(i)])
        return carry

    lax.fori_loop(0, 2 * n_chunks, prepare_own, 0)

    per_phase = 3 * n_chunks
    steps = 2 * per_phase

    def facts(s):
        phase = lax.div(s, per_phase)
        h = lax.div(lax.rem(s, per_phase), 3)
        j = lax.rem(s, 3)
        is_edge = (phase == 1) & (j != 1)
        slot = jnp.where(phase == 0, j, jnp.where(j == 0, 1, 3))
        ahead = jnp.where(slot == 1, 1, jnp.where(slot == 2, -1, jnp.where(slot == 3, 2, 0)))
        tile = z + step_z * ahead
        active = (s >= 0) & (s < steps) & (inner | ((phase == 0) & (j < 2)))
        tile_x, tile_y = lax.rem(tile + 4, 2), lax.rem(lax.div(tile + 4, 2), 2)
        off_x, off_y = flip(tile_x, x), flip(tile_y, y)
        return h, slot, is_edge, active, off_x, off_y

    low, high = pl.ds(0, half), pl.ds(half, half)

    def far_copy(s, k, h):
        cols = (low, high)[k]
        return remote(sent.at[lax.rem(s, SLOTS), :, cols], far_in.at[k, h],
                      stage_send.at[lax.rem(s, SLOTS), k], far_recv.at[k, h],
                      (x_peer, y_peer)[k], z)

    def near_copy(s, k, h):
        cols = (low, high)[k]
        return remote(sent.at[lax.rem(s, SLOTS), :, cols], near_in.at[k, h],
                      stage_send.at[lax.rem(s, SLOTS), k], near_recv.at[k, h],
                      (x_peer, y_peer)[k], z)

    def last_copy(s, k, h):
        cols = (low, high)[k]
        return remote(joined.at[lax.rem(s, SLOTS), :, cols], last_in.at[k, h],
                      join_send.at[lax.rem(s, SLOTS), k], last_recv.at[k, h],
                      (y_peer, x_peer)[k], z)

    def edge_copy(s, h):
        return remote(sent.at[lax.rem(s, SLOTS)], outer_in.at[h],
                      stage_send.at[lax.rem(s, SLOTS), 0], outer_recv.at[h], x_peer, z)

    def sums_copy(s, h):
        return remote(joined.at[lax.rem(s, SLOTS)], sums_ref.at[rows_of(h)],
                      join_send.at[lax.rem(s, SLOTS), 0], sums_recv.at[h], me, away_z)

    def relay_copy(h):
        return remote(sums_ref.at[rows_of(h)], last_sums_ref.at[rows_of(h)],
                      relay_send.at[h], relay_recv.at[h], y_peer, z)

    def out_copy(s, h):
        return pltpu.make_async_copy(
            partial.at[lax.rem(s, SLOTS)], out_ref.at[rows_of(h)], store_sem)

    def compute(s):
        h, slot, is_edge, active, off_x, off_y = facts(s)

        @pl.when(active)
        def _():
            @pl.when((slot == 1) & jnp.logical_not(is_edge))
            def _():
                arrived(0, h).wait_recv()

            @pl.when(slot == 2)
            def _():
                arrived(1, h).wait_recv()
                send_on(h).start()
                send_twin(h).start()

            @pl.when((slot == 3) & jnp.logical_not(is_edge))
            def _():
                arrived(2, h).wait_recv()

            @pl.when(slot == 0)
            def _():
                load(both_ref.at[own_rows(h)], left)

            @pl.when(slot > 0)
            def _():
                load(held_ref.at[jnp.where(slot == 0, 0, slot - 1), rows_of(h)], left)

            kind = jnp.where(is_edge, 1, 0)
            buf = lax.rem(s, SLOTS)

            def tile_product(n, carry):
                cols = pl.ds(pl.multiple_of(n * 256, 256), 256)
                partial[buf, :, cols] = lax.dot_general(
                    left[...], right[kind, cols, :], (((1,), (1,)), ((), ())),
                    preferred_element_type=jnp.float32,
                )
                return carry

            lax.fori_loop(0, n_cols // 256, tile_product, 0)

            plain = jnp.logical_not(is_edge)

            def round_half(cols):
                sent[buf, :, cols] = partial[buf, :, cols].astype(jnp.bfloat16)

            @pl.when(plain & (off_x == 1) & (off_y == 1))
            def _():
                round_half(low)
                far_copy(s, 0, h).start()
                round_half(high)
                far_copy(s, 1, h).start()

            @pl.when(plain & (off_x == 1) & (off_y == 0))
            def _():
                round_half(low)
                near_copy(s, 0, h).start()

            @pl.when(plain & (off_x == 0) & (off_y == 1))
            def _():
                round_half(high)
                near_copy(s, 1, h).start()

            @pl.when(is_edge & (off_x == 1))
            def _():
                round_half(low)
                round_half(high)
                edge_copy(s, h).start()

    def join(s):
        h, slot, is_edge, active, off_x, off_y = facts(s)
        buf = lax.rem(jnp.maximum(s, 0), SLOTS)
        plain = jnp.logical_not(is_edge)

        def add(cols, value):
            joined[buf, :, cols] = (
                partial[buf, :, cols] + value.astype(jnp.float32)
            ).astype(jnp.bfloat16)

        @pl.when(active & plain & (off_x == 1) & (off_y == 0))
        def _():
            far_copy(s, 1, h).wait_recv()
            add(high, far_in[1, h])
            last_copy(s, 1, h).start()

        @pl.when(active & plain & (off_x == 0) & (off_y == 1))
        def _():
            far_copy(s, 0, h).wait_recv()
            add(low, far_in[0, h])
            last_copy(s, 0, h).start()

        @pl.when(active & is_edge & (off_x == 0))
        def _():
            edge_copy(s, h).wait_recv()
            add(low, outer_in[h, :, low])
            add(high, outer_in[h, :, high])
            sums_copy(s, h).start()

    def finish(s):
        h, slot, is_edge, active, off_x, off_y = facts(s)
        buf = lax.rem(jnp.maximum(s, 0), SLOTS)
        plain = jnp.logical_not(is_edge)

        @pl.when(active & plain & (off_x == 0) & (off_y == 0))
        def _():
            for k, cols in ((0, low), (1, high)):
                near_copy(s, k, h).wait_recv()
                last_copy(s, k, h).wait_recv()
                partial[buf, :, cols] = (
                    partial[buf, :, cols]
                    + near_in[k, h].astype(jnp.float32)
                    + last_in[k, h].astype(jnp.float32)
                )
            out_copy(s, h).start()
            out_copy(s, h).wait()

        @pl.when(active & plain & (off_x == 1) & (off_y == 1))
        def _():
            far_copy(s, 0, h).wait_send()
            far_copy(s, 1, h).wait_send()

        @pl.when(active & plain & (off_x == 1) & (off_y == 0))
        def _():
            near_copy(s, 0, h).wait_send()
            last_copy(s, 1, h).wait_send()

        @pl.when(active & plain & (off_x == 0) & (off_y == 1))
        def _():
            near_copy(s, 1, h).wait_send()
            last_copy(s, 0, h).wait_send()

        @pl.when(active & is_edge & (off_x == 1))
        def _():
            edge_copy(s, h).wait_send()

        @pl.when(active & is_edge & (off_x == 0))
        def _():
            sums_copy(s, h).wait_send()

    def one_step(s, carry):
        @pl.when(s == per_phase)
        def _():
            @pl.when(inner)
            def _():
                def prepare(h, carry):
                    send_twin(h).wait_recv()
                    weigh_into(1, core * half + h * chunk, held_ref.at[1, rows_of(h)])
                    weigh_into(1, (1 - core) * half + h * chunk, twin_ref.at[rows_of(h)])
                    return carry

                lax.fori_loop(0, n_chunks, prepare, 0)

        @pl.when(s < steps)
        def _():
            compute(s)

        join(s - LAG_JOIN)
        finish(s - LAG_OUT)
        return carry

    lax.fori_loop(0, steps + LAG_OUT, one_step, 0)

    owner_y = jnp.where(side == 0, 1, 0)

    @pl.when(outer)
    def _():
        for h in range(n_chunks):
            remote(sums_ref.at[rows_of(h)], sums_ref.at[rows_of(h)],
                   sums_send.at[0], sums_recv.at[h], me, toward_z).wait_recv()

            @pl.when(y != owner_y)
            def _():
                relay_copy(h).start()

        for h in range(n_chunks):
            @pl.when(y != owner_y)
            def _():
                relay_copy(h).wait_send()

            @pl.when(y == owner_y)
            def _():
                relay_copy(h).wait_recv()

    for h in range(n_chunks):
        send_toward(h).wait_send()

        @pl.when(inner)
        def _():
            send_away(h).wait_send()
            send_on(h).wait_send()
            send_twin(h).wait_send()


def line(design, observations, solution, arc_ids, block_live):
    me, z = lax.axis_index("arcs"), lax.axis_index("tiles")
    core, y = lax.rem(me, 2), lax.div(me, 4)
    rows, columns = design.shape
    half = columns // 2
    chunks = half // STEP_ROWS
    pairs = [(i, i ^ 1) for i in range(8)]

    turned = design.T
    turned_peer = lax.ppermute(turned, "arcs", pairs)
    row_weight, residual = row_weights(design, observations, solution, arc_ids, block_live)
    rhs = lax.psum(right_side(design, row_weight, residual), "arcs")
    weight_peer = lax.ppermute(row_weight, "arcs", pairs)
    first = core == 0
    both = jnp.concatenate(
        [jnp.where(first, turned, turned_peer), jnp.where(first, turned_peer, turned)], axis=1
    )
    weight = jnp.concatenate(
        [jnp.where(first, row_weight, weight_peer), jnp.where(first, weight_peer, row_weight)]
    )[None, :]

    half_dtype, wide = jnp.bfloat16, jnp.float32
    shape = jax.ShapeDtypeStruct
    dma = pltpu.SemaphoreType.DMA
    own, held, twin, sums, last_sums = pl.pallas_call(
        line_kernel,
        out_shape=(
            shape((half, columns), wide),
            shape((3, half, 2 * rows), half_dtype),
            shape((half, 2 * rows), half_dtype),
            shape((half, columns), half_dtype),
            shape((half, columns), half_dtype),
        ),
        in_specs=[
            pl.BlockSpec(memory_space=pl.ANY),
            pl.BlockSpec(memory_space=pltpu.VMEM),
        ],
        out_specs=[pl.BlockSpec(memory_space=pl.ANY)] * 5,
        scratch_shapes=[
            pltpu.VMEM((2, columns, 2 * rows), half_dtype),
            pltpu.VMEM((STEP_ROWS, 2 * rows), half_dtype),
            pltpu.VMEM((SLOTS, STEP_ROWS, columns), wide),
            pltpu.VMEM((SLOTS, STEP_ROWS, columns), half_dtype),
            pltpu.VMEM((SLOTS, STEP_ROWS, columns), half_dtype),
            pltpu.VMEM((2, chunks, STEP_ROWS, half), half_dtype),
            pltpu.VMEM((2, chunks, STEP_ROWS, half), half_dtype),
            pltpu.VMEM((2, chunks, STEP_ROWS, half), half_dtype),
            pltpu.VMEM((chunks, STEP_ROWS, columns), half_dtype),
            dma, dma,
            dma((chunks,)), dma((chunks,)), dma((chunks,)), dma((chunks,)),
            dma((3, chunks)), dma((chunks,)),
            dma((SLOTS, 2)), dma((SLOTS, 2)),
            dma((2, chunks)), dma((2, chunks)), dma((2, chunks)), dma((chunks,)),
            dma((1,)), dma((chunks,)), dma((chunks,)), dma((chunks,)),
        ],
        compiler_params=pltpu.CompilerParams(
            collective_id=0, has_side_effects=True, vmem_limit_bytes=67_000_000
        ),
    )(both, weight)
    is_outer_owner = ((z == 0) & (y == 1)) | ((z == 3) & (y == 0))
    normal = jnp.where(is_outer_owner, sums.astype(wide) + last_sums.astype(wide), own)
    return (normal, rhs)


def solution(mesh):
    n_arcs, n_tiles = mesh.shape["arcs"], mesh.shape["tiles"]

    def local(design, *rest):
        fits = design.shape[1] % (4 * STEP_ROWS) == 0
        if n_arcs == 8 and n_tiles == 4 and fits:
            return line(design, *rest)
        return general(design, *rest)

    return jax.shard_map(
        local,
        mesh=mesh,
        in_specs=(P("arcs", "tiles"), P("arcs"), P("tiles"), P("arcs", None), P("arcs", None)),
        out_specs=(P("arcs", "tiles"), P("tiles")),
        check_vma=False,
    )
```

```python
import functools

import jax
import jax.numpy as jnp
from jax import lax
from jax.experimental import pallas as pl
from jax.experimental.pallas import tpu as pltpu
from jax.sharding import PartitionSpec as P

ARCS_DEV = 4
STEP_ROWS = 256
LAG_JOIN = 2
LAG_OUT = 5
SLOTS = 5
JOINED = 3
MESH = pl.DeviceIdType.MESH

prior_rows = 4.0


def contract_rows(left, right):
    return lax.dot_general(
        left, right, (((0,), (0,)), ((), ())), preferred_element_type=jnp.float32
    )


def row_weights(design, observations, solution, arc_ids, block_live, early=()):
    row_count = design.shape[0]
    partial_value = jnp.dot(design.astype(jnp.float32), solution, precision=lax.Precision.HIGHEST)
    predicted = lax.psum(partial_value, "tiles")
    predicted, early = lax.optimization_barrier((predicted, early))
    residual = observations - predicted
    live_row = (
        jnp.broadcast_to(block_live[0][:, None], (block_live.shape[1], 128))
        .reshape(row_count)
        .astype(jnp.float32)
    )
    arc_match = (arc_ids[0][None, :] == jnp.arange(ARCS_DEV, dtype=jnp.int32)[:, None]).astype(
        jnp.float32
    )
    squares = live_row * residual * residual
    arc_squares = jnp.sum(arc_match * squares[None, :], axis=1)
    arc_counts = jnp.sum(arc_match * live_row[None, :], axis=1)
    totals = lax.psum(jnp.stack([jnp.sum(arc_squares), jnp.sum(arc_counts)]), "arcs")
    variance_all = (totals[0] + 1.0) / (totals[1] + 1.0)
    arc_weight = variance_all / (
        (arc_squares + prior_rows * variance_all) / (arc_counts + prior_rows)
    )
    row_weight = live_row * jnp.sum(arc_match * arc_weight[:, None], axis=0)
    return row_weight, residual, early


def right_side(design, row_weight, residual):
    return lax.dot_general(
        design.astype(jnp.float32),
        row_weight * residual,
        (((0,), (0,)), ((), ())),
        precision=lax.Precision.HIGHEST,
    )


def general(design, observations, solution, arc_ids, block_live):
    design_all = lax.all_gather(design, "tiles", axis=1, tiled=True)
    row_weight, residual, _ = row_weights(design, observations, solution, arc_ids, block_live)
    rhs = lax.psum(right_side(design, row_weight, residual), "arcs")
    weighted = (row_weight[:, None] * design).astype(jnp.bfloat16)
    normal = lax.psum_scatter(
        contract_rows(design_all, weighted), "arcs", scatter_dimension=0, tiled=True
    )
    return (normal, rhs)


def line_kernel(
    both_ref, weight_ref, rhs_ref, toward_ref, away_ref,
    out_ref, held_ref, twin_ref, sums_ref, last_sums_ref, rhs_out_ref,
    right, left, rhs_in, partial, sent, joined, far_in, near_in, last_in, outer_in,
    load_sem, store_sem, prep_sem, a_send, w_send, b_send, twin_send, held_recv, twin_recv,
    stage_send, join_send, far_recv, near_recv, last_recv, outer_recv,
    sums_recv, relay_send, relay_recv, rhs_send, rhs_recv,
):
    n_cols, n_rows = both_ref.shape
    half = n_cols // 2
    chunk = STEP_ROWS
    n_chunks = half // chunk
    me, z = lax.axis_index("arcs"), lax.axis_index("tiles")
    core, chip = lax.rem(me, 2), lax.div(me, 2)
    x, y = lax.rem(chip, 2), lax.div(chip, 2)
    x_peer = me + 2 - 4 * x
    y_peer = me + 4 - 8 * y
    core_peer = me + 1 - 2 * core
    side = lax.div(z, 2)
    step_z = 1 - 2 * side
    inner = (z == 1) | (z == 2)
    outer = jnp.logical_not(inner)
    toward_z = z + step_z
    away_z = jnp.where(inner, z - step_z, z)

    def flip(a, b):
        return a + b - 2 * a * b

    def rows_of(h):
        return pl.ds(pl.multiple_of(h * chunk, chunk), chunk)

    def own_rows(h):
        return pl.ds(pl.multiple_of(core * half + h * chunk, chunk), chunk)

    def remote(src, dst, send, recv, a, zz):
        return pltpu.make_async_remote_copy(
            src_ref=src, dst_ref=dst, send_sem=send, recv_sem=recv,
            device_id=(a, zz), device_id_type=MESH,
        )

    def send_toward(h):
        slot = jnp.where(inner, 0, 1)
        return remote(both_ref.at[own_rows(h)], held_ref.at[slot, rows_of(h)],
                      a_send.at[h], held_recv.at[slot, h], me, toward_z)

    def send_away(h):
        return remote(both_ref.at[own_rows(h)], held_ref.at[0, rows_of(h)],
                      w_send.at[h], held_recv.at[0, h], me, away_z)

    def send_on(h):
        return remote(held_ref.at[1, rows_of(h)], held_ref.at[2, rows_of(h)],
                      b_send.at[h], held_recv.at[2, h], me, toward_z)

    def send_twin(h):
        return remote(held_ref.at[1, rows_of(h)], twin_ref.at[rows_of(h)],
                      twin_send.at[h], twin_recv.at[h], core_peer, z)

    def send_first_twin():
        return remote(away_ref, twin_ref.at[rows_of(0)],
                      twin_send.at[0], twin_recv.at[0], core_peer, z)

    def send_first_on():
        return remote(away_ref, held_ref.at[2, rows_of(0)],
                      b_send.at[0], held_recv.at[2, 0], me, toward_z)

    def rhs_copy(k):
        return remote(rhs_ref, rhs_in.at[k], rhs_send.at[k], rhs_recv.at[k],
                      lax.rem(me + k + 1, 8), z)

    def arrived(slot, h):
        return remote(held_ref.at[slot, rows_of(h)], held_ref.at[slot, rows_of(h)],
                      a_send.at[h], held_recv.at[slot, h], me, toward_z)

    barrier = pltpu.get_barrier_semaphore()
    for k in range(7):
        pl.semaphore_signal(barrier, inc=1, device_id=(lax.rem(me + k + 1, 8), z),
                            device_id_type=MESH)
    pl.semaphore_signal(barrier, inc=1, device_id=(me, toward_z), device_id_type=MESH)

    @pl.when(inner)
    def _():
        pl.semaphore_signal(barrier, inc=1, device_id=(me, away_z), device_id_type=MESH)
        pl.semaphore_wait(barrier, 9)

    @pl.when(outer)
    def _():
        pl.semaphore_wait(barrier, 8)

    @pl.when(inner)
    def _():
        send_first_on().start()

    for h in range(1, n_chunks):
        @pl.when(outer | (h < 3))
        def _():
            send_toward(h).start()

        @pl.when(inner)
        def _():
            send_away(h).start()

    for k in range(7):
        rhs_copy(k).start()

    def load(src, dst):
        copy = pltpu.make_async_copy(src, dst, load_sem)
        copy.start()
        copy.wait()

    def weigh_into(kind, first):
        def body(i, carry):
            rows = pl.ds(pl.multiple_of(i * 32, 32), 32)
            value = left[rows, :].astype(jnp.float32) * weight_ref[...]
            at = pl.ds(pl.multiple_of(first + i * 32, 32), 32)
            right[kind, at, :] = value.astype(jnp.bfloat16)
            return carry

        lax.fori_loop(0, chunk // 32, body, 0)

    def stage_own(i):
        rows = rows_of(i)
        return pltpu.make_async_copy(both_ref.at[rows], right.at[1, rows], prep_sem.at[i])

    def prepare_own(i, carry):
        stage_own(i).wait()

        def body(k, carry):
            rows = pl.ds(pl.multiple_of(i * chunk + k * 32, 32), 32)
            value = right[1, rows, :].astype(jnp.float32) * weight_ref[...]
            right[0, rows, :] = value.astype(jnp.bfloat16)
            return carry

        lax.fori_loop(0, chunk // 32, body, 0)
        return carry

    for i in range(2 * n_chunks):
        stage_own(i).start()

    def load_twin(h):
        mine = n_rows // 2
        for src, dst in ((0, mine), (mine, 0)):
            load(twin_ref.at[rows_of(h), pl.ds(src, mine)], left.at[:, pl.ds(dst, mine)])

    def serve_away(h):
        arrived(1, h).wait_recv()
        send_on(h).start()
        send_twin(h).start()

        @pl.when(h == 1)
        def _():
            send_toward(3).start()

        load(held_ref.at[1, rows_of(h)], left)
        weigh_into(1, core * half + h * chunk)
        send_twin(h).wait_recv()
        load_twin(h)
        weigh_into(1, (1 - core) * half + h * chunk)

    def serve_first_away():
        send_first_twin().start()
        load(away_ref, left)
        weigh_into(1, core * half)
        send_first_twin().wait_recv()
        load_twin(0)
        weigh_into(1, (1 - core) * half)

    lax.fori_loop(0, 2 * n_chunks, prepare_own, 0)

    own, near, back, far = 0, 1, 2, 3
    order = (
        (back, 0, 0), (near, 0, 0), (own, 0, 0), (far, 0, 0), (back, 1, 0), (near, 1, 0),
        (own, 1, 0), (back, 2, 0), (near, 0, 1), (far, 0, 1), (near, 1, 1), (near, 2, 0),
        (own, 2, 0), (far, 1, 0), (far, 1, 1), (back, 3, 0), (near, 2, 1), (own, 3, 0),
        (near, 3, 0), (near, 3, 1), (far, 2, 0), (far, 2, 1), (far, 3, 1), (far, 3, 0),
    )
    steps = len(order)
    first_edge = 8

    def facts(s):
        code = jnp.int32(0)
        for i, (slot, h, edge) in enumerate(order):
            code = code + jnp.where(s == i, slot * 8 + h * 2 + edge, 0)
        slot, h = lax.div(code, 8), lax.rem(lax.div(code, 2), 4)
        is_edge = lax.rem(code, 2) == 1
        ahead = jnp.where(slot == 1, 1, jnp.where(slot == 2, -1, jnp.where(slot == 3, 2, 0)))
        tile = z + step_z * ahead
        plain_near = (slot < 2) & jnp.logical_not(is_edge)
        active = (s >= 0) & (s < steps) & (inner | plain_near)
        tile_x, tile_y = lax.rem(tile + 4, 2), lax.rem(lax.div(tile + 4, 2), 2)
        off_x, off_y = flip(tile_x, x), flip(tile_y, y)
        return h, slot, is_edge, active, off_x, off_y

    low, high = pl.ds(0, half), pl.ds(half, half)

    def far_copy(s, k, h):
        cols = (low, high)[k]
        return remote(sent.at[lax.rem(s, SLOTS), :, cols], far_in.at[k, h],
                      stage_send.at[lax.rem(s, SLOTS), k], far_recv.at[k, h],
                      (x_peer, y_peer)[k], z)

    def near_copy(s, k, h):
        cols = (low, high)[k]
        return remote(sent.at[lax.rem(s, SLOTS), :, cols], near_in.at[k, h],
                      stage_send.at[lax.rem(s, SLOTS), k], near_recv.at[k, h],
                      (x_peer, y_peer)[k], z)

    def last_copy(s, k, h):
        cols = (low, high)[k]
        return remote(joined.at[lax.rem(s, JOINED), :, cols], last_in.at[k, h],
                      join_send.at[lax.rem(s, JOINED), k], last_recv.at[k, h],
                      (y_peer, x_peer)[k], z)

    def edge_copy(s, k, h):
        cols = (low, high)[k]
        return remote(sent.at[lax.rem(s, SLOTS), :, cols], outer_in.at[k, h],
                      stage_send.at[lax.rem(s, SLOTS), k], outer_recv.at[k, h], x_peer, z)

    def sums_copy(s, k, h):
        cols = (low, high)[k]
        return remote(joined.at[lax.rem(s, JOINED), :, cols], sums_ref.at[rows_of(h), (low, high)[k]],
                      join_send.at[lax.rem(s, JOINED), k], sums_recv.at[k, h], me, away_z)

    def relay_copy(k, h):
        return remote(sums_ref.at[rows_of(h), (low, high)[k]], last_sums_ref.at[rows_of(h), (low, high)[k]],
                      relay_send.at[k, h], relay_recv.at[k, h], y_peer, z)

    def out_copy(s, h):
        return pltpu.make_async_copy(
            partial.at[lax.rem(s, SLOTS)], out_ref.at[rows_of(h)], store_sem)

    def compute(s):
        h, slot, is_edge, active, off_x, off_y = facts(s)

        @pl.when(active)
        def _():
            plain = jnp.logical_not(is_edge)

            @pl.when((slot == 1) & plain & (h > 0))
            def _():
                arrived(0, h).wait_recv()

            @pl.when((slot == 2) & (h == 0))
            def _():
                serve_first_away()

            @pl.when((slot == 2) & (h > 0) & (h < 3))
            def _():
                serve_away(h)

            @pl.when(s == first_edge)
            def _():
                serve_away(3)

            @pl.when((slot == 3) & (plain != (h == 3)))
            def _():
                arrived(2, h).wait_recv()

            @pl.when(slot == 0)
            def _():
                load(both_ref.at[own_rows(h)], left)

            @pl.when((slot == 3) | ((slot > 0) & (h > 0)))
            def _():
                load(held_ref.at[jnp.maximum(slot - 1, 0), rows_of(h)], left)

            for k, first_ref in enumerate((toward_ref, away_ref)):
                @pl.when((slot == k + 1) & (h == 0))
                def _():
                    load(first_ref, left)

            kind = jnp.where(is_edge, 1, 0)
            buf = lax.rem(s, SLOTS)

            def tile_product(n, carry):
                cols = pl.ds(pl.multiple_of(n * 512, 512), 512)
                partial[buf, :, cols] = lax.dot_general(
                    left[...], right[kind, cols, :], (((1,), (1,)), ((), ())),
                    preferred_element_type=jnp.float32,
                )
                return carry

            tiles = n_cols // 512
            lax.fori_loop(0, tiles // 2, tile_product, 0)

            def round_half(cols):
                sent[buf, :, cols] = partial[buf, :, cols].astype(jnp.bfloat16)

            @pl.when(plain & (off_x == 1) & (off_y == 1))
            def _():
                round_half(low)
                far_copy(s, 0, h).start()

            @pl.when(plain & (off_x == 1) & (off_y == 0))
            def _():
                round_half(low)
                near_copy(s, 0, h).start()

            @pl.when(is_edge & (off_x == 1))
            def _():
                round_half(low)
                edge_copy(s, 0, h).start()

            lax.fori_loop(tiles // 2, tiles, tile_product, 0)

            @pl.when(plain & (off_x == 1) & (off_y == 1))
            def _():
                round_half(high)
                far_copy(s, 1, h).start()

            @pl.when(plain & (off_x == 0) & (off_y == 1))
            def _():
                round_half(high)
                near_copy(s, 1, h).start()

            @pl.when(is_edge & (off_x == 1))
            def _():
                round_half(high)
                edge_copy(s, 1, h).start()

    def join(s):
        h, slot, is_edge, active, off_x, off_y = facts(s)
        buf = lax.rem(jnp.maximum(s, 0), SLOTS)
        place = lax.rem(jnp.maximum(s, 0), JOINED)
        plain = jnp.logical_not(is_edge)

        def add(cols, value):
            joined[place, :, cols] = (
                partial[buf, :, cols] + value.astype(jnp.float32)
            ).astype(jnp.bfloat16)

        @pl.when(active & plain & (off_x == 1) & (off_y == 0))
        def _():
            far_copy(s, 1, h).wait_recv()
            add(high, far_in[1, h])
            last_copy(s, 1, h).start()

        @pl.when(active & plain & (off_x == 0) & (off_y == 1))
        def _():
            far_copy(s, 0, h).wait_recv()
            add(low, far_in[0, h])
            last_copy(s, 0, h).start()

        @pl.when(active & is_edge & (off_x == 0))
        def _():
            for k, cols in ((0, low), (1, high)):
                edge_copy(s, k, h).wait_recv()
                add(cols, outer_in[k, h])
                sums_copy(s, k, h).start()

    def finish(s):
        h, slot, is_edge, active, off_x, off_y = facts(s)
        buf = lax.rem(jnp.maximum(s, 0), SLOTS)
        plain = jnp.logical_not(is_edge)

        @pl.when(active & plain & (off_x == 0) & (off_y == 0))
        def _():
            for k, cols in ((0, low), (1, high)):
                near_copy(s, k, h).wait_recv()
                last_copy(s, k, h).wait_recv()
                partial[buf, :, cols] = (
                    partial[buf, :, cols]
                    + near_in[k, h].astype(jnp.float32)
                    + last_in[k, h].astype(jnp.float32)
                )
            out_copy(s, h).start()
            out_copy(s, h).wait()

        @pl.when(active & plain & (off_x == 1) & (off_y == 1))
        def _():
            far_copy(s, 0, h).wait_send()
            far_copy(s, 1, h).wait_send()

        @pl.when(active & plain & (off_x == 1) & (off_y == 0))
        def _():
            near_copy(s, 0, h).wait_send()
            last_copy(s, 1, h).wait_send()

        @pl.when(active & plain & (off_x == 0) & (off_y == 1))
        def _():
            near_copy(s, 1, h).wait_send()
            last_copy(s, 0, h).wait_send()

        @pl.when(active & is_edge & (off_x == 1))
        def _():
            edge_copy(s, 0, h).wait_send()
            edge_copy(s, 1, h).wait_send()

        @pl.when(active & is_edge & (off_x == 0))
        def _():
            sums_copy(s, 0, h).wait_send()
            sums_copy(s, 1, h).wait_send()

    def one_step(s, carry):
        finish(s - LAG_OUT)

        @pl.when(s < steps)
        def _():
            compute(s)

        join(s - LAG_JOIN)
        return carry

    lax.fori_loop(0, steps + LAG_OUT, one_step, 0)

    owner_y = jnp.where(side == 0, 1, 0)

    @pl.when(outer)
    def _():
        for h in range(n_chunks):
            for k in range(2):
                remote(sums_ref.at[rows_of(h), (low, high)[k]], sums_ref.at[rows_of(h), (low, high)[k]],
                       relay_send.at[k, h], sums_recv.at[k, h], me, toward_z).wait_recv()

                @pl.when(y != owner_y)
                def _():
                    relay_copy(k, h).start()

        for h in range(n_chunks):
            for k in range(2):
                @pl.when(y != owner_y)
                def _():
                    relay_copy(k, h).wait_send()

                @pl.when(y == owner_y)
                def _():
                    relay_copy(k, h).wait_recv()

    @pl.when(inner)
    def _():
        send_first_twin().wait_send()
        send_first_on().wait_send()

    for h in range(1, n_chunks):
        send_toward(h).wait_send()

        @pl.when(inner)
        def _():
            send_away(h).wait_send()
            send_on(h).wait_send()
            send_twin(h).wait_send()

    total = rhs_ref[...]
    for k in range(7):
        rhs_copy(k).wait()
        total = total + rhs_in[k]
    rhs_out_ref[...] = total


def line(design, observations, solution, arc_ids, block_live):
    me, z = lax.axis_index("arcs"), lax.axis_index("tiles")
    core, y = lax.rem(me, 2), lax.div(me, 4)
    rows, columns = design.shape
    half = columns // 2
    chunks = half // STEP_ROWS
    pairs = [(i, i ^ 1) for i in range(8)]

    def in_order(mine, peers):
        return jnp.concatenate([mine, peers], axis=-1)

    turned = design.T
    own_first = lax.dynamic_slice_in_dim(turned, core * half, STEP_ROWS, 0)
    give_first = lax.dynamic_slice_in_dim(turned, (1 - core) * half, STEP_ROWS, 0)
    own_first = in_order(own_first, lax.ppermute(give_first, "arcs", pairs))
    turned, design, own_first = lax.optimization_barrier((turned, design, own_first))
    turned_peer = lax.ppermute(turned, "arcs", pairs)
    row_weight, residual, own_first = row_weights(
        design, observations, solution, arc_ids, block_live, own_first
    )
    below = lax.ppermute(own_first, "tiles", [(0, 1), (1, 2), (2, 3)])
    above = lax.ppermute(own_first, "tiles", [(1, 0), (2, 1), (3, 2)])
    toward = jnp.where(z < 2, above, below)
    away = jnp.where(z < 2, below, above)
    rhs_part = right_side(design, row_weight, residual).reshape(-1, 128)
    weight = in_order(row_weight, lax.ppermute(row_weight, "arcs", pairs))[None, :]
    both = in_order(turned, turned_peer)

    half_dtype, wide = jnp.bfloat16, jnp.float32
    shape = jax.ShapeDtypeStruct
    dma = pltpu.SemaphoreType.DMA
    own, held, twin, sums, last_sums, rhs = pl.pallas_call(
        line_kernel,
        out_shape=(
            shape((half, columns), wide),
            shape((3, half, 2 * rows), half_dtype),
            shape((half, 2 * rows), half_dtype),
            shape((half, columns), half_dtype),
            shape((half, columns), half_dtype),
            shape(rhs_part.shape, wide),
        ),
        in_specs=[
            pl.BlockSpec(memory_space=pl.ANY),
            pl.BlockSpec(memory_space=pltpu.VMEM),
            pl.BlockSpec(memory_space=pltpu.VMEM),
        ]
        + [pl.BlockSpec(memory_space=pl.ANY)] * 2,
        out_specs=[pl.BlockSpec(memory_space=pl.ANY)] * 5
        + [pl.BlockSpec(memory_space=pltpu.VMEM)],
        scratch_shapes=[
            pltpu.VMEM((2, columns, 2 * rows), half_dtype),
            pltpu.VMEM((STEP_ROWS, 2 * rows), half_dtype),
            pltpu.VMEM((7,) + rhs_part.shape, wide),
            pltpu.VMEM((SLOTS, STEP_ROWS, columns), wide),
            pltpu.VMEM((SLOTS, STEP_ROWS, columns), half_dtype),
            pltpu.VMEM((JOINED, STEP_ROWS, columns), half_dtype),
            pltpu.VMEM((2, chunks, STEP_ROWS, half), half_dtype),
            pltpu.VMEM((2, chunks, STEP_ROWS, half), half_dtype),
            pltpu.VMEM((2, chunks, STEP_ROWS, half), half_dtype),
            pltpu.VMEM((2, chunks, STEP_ROWS, half), half_dtype),
            dma, dma, dma((2 * chunks,)),
            dma((chunks,)), dma((chunks,)), dma((chunks,)), dma((chunks,)),
            dma((3, chunks)), dma((chunks,)),
            dma((SLOTS, 2)), dma((JOINED, 2)),
            dma((2, chunks)), dma((2, chunks)), dma((2, chunks)), dma((2, chunks)),
            dma((2, chunks)), dma((2, chunks)), dma((2, chunks)), dma((7,)), dma((7,)),
        ],
        compiler_params=pltpu.CompilerParams(
            collective_id=0, has_side_effects=True, vmem_limit_bytes=67_000_000
        ),
    )(both, weight, rhs_part, toward, away)
    edge = sums.astype(wide) + last_sums.astype(wide)
    is_outer_owner = ((z == 0) & (y == 1)) | ((z == 3) & (y == 0))
    normal = jnp.where(is_outer_owner, edge, own)
    return (normal, rhs.reshape(-1))


def solution(mesh):
    n_arcs, n_tiles = mesh.shape["arcs"], mesh.shape["tiles"]

    def local(design, *rest):
        fits = design.shape[1] == 8 * STEP_ROWS and design.shape[1] % 128 == 0
        if n_arcs == 8 and n_tiles == 4 and fits:
            return line(design, *rest)
        return general(design, *rest)

    return jax.shard_map(
        local,
        mesh=mesh,
        in_specs=(P("arcs", "tiles"), P("arcs"), P("tiles"), P("arcs", None), P("arcs", None)),
        out_specs=(P("arcs", "tiles"), P("tiles")),
        check_vma=False,
    )
```

```python
import functools

import jax
import jax.numpy as jnp
from jax import lax
from jax.experimental import pallas as pl
from jax.experimental.pallas import tpu as pltpu
from jax.sharding import PartitionSpec as P

ARCS_DEV = 4
STEP_ROWS = 256
LAG_JOIN = 2
LAG_OUT = 5
SLOTS = 5
JOINED = 3
MESH = pl.DeviceIdType.MESH

prior_rows = 4.0


def contract_rows(left, right):
    return lax.dot_general(
        left, right, (((0,), (0,)), ((), ())), preferred_element_type=jnp.float32
    )


def row_weights(design, observations, solution, arc_ids, block_live, early=()):
    row_count = design.shape[0]
    partial_value = jnp.dot(design.astype(jnp.float32), solution, precision=lax.Precision.HIGHEST)
    predicted = lax.psum(partial_value, "tiles")
    predicted, early = lax.optimization_barrier((predicted, early))
    residual = observations - predicted
    live_row = (
        jnp.broadcast_to(block_live[0][:, None], (block_live.shape[1], 128))
        .reshape(row_count)
        .astype(jnp.float32)
    )
    arc_match = (arc_ids[0][None, :] == jnp.arange(ARCS_DEV, dtype=jnp.int32)[:, None]).astype(
        jnp.float32
    )
    squares = live_row * residual * residual
    arc_squares = jnp.sum(arc_match * squares[None, :], axis=1)
    arc_counts = jnp.sum(arc_match * live_row[None, :], axis=1)
    totals = lax.psum(jnp.stack([jnp.sum(arc_squares), jnp.sum(arc_counts)]), "arcs")
    variance_all = (totals[0] + 1.0) / (totals[1] + 1.0)
    arc_weight = variance_all / (
        (arc_squares + prior_rows * variance_all) / (arc_counts + prior_rows)
    )
    row_weight = live_row * jnp.sum(arc_match * arc_weight[:, None], axis=0)
    return row_weight, residual, early


def right_side(design, row_weight, residual):
    return lax.dot_general(
        design.astype(jnp.float32),
        row_weight * residual,
        (((0,), (0,)), ((), ())),
        precision=lax.Precision.HIGHEST,
    )


def general(design, observations, solution, arc_ids, block_live):
    design_all = lax.all_gather(design, "tiles", axis=1, tiled=True)
    row_weight, residual, _ = row_weights(design, observations, solution, arc_ids, block_live)
    rhs = lax.psum(right_side(design, row_weight, residual), "arcs")
    weighted = (row_weight[:, None] * design).astype(jnp.bfloat16)
    normal = lax.psum_scatter(
        contract_rows(design_all, weighted), "arcs", scatter_dimension=0, tiled=True
    )
    return (normal, rhs)


def line_kernel(
    both_ref, weight_ref, rhs_ref, below_ref, above_ref,
    out_ref, held_ref, twin_ref, sums_ref, last_sums_ref, rhs_out_ref,
    right, left, rhs_in, partial, sent, joined, far_in, near_in, last_in, outer_in,
    load_sem, store_sem, prep_sem, a_send, w_send, b_send, twin_send, held_recv, twin_recv,
    stage_send, join_send, far_recv, near_recv, last_recv, outer_recv,
    sums_recv, relay_send, relay_recv, rhs_send, rhs_recv,
):
    n_cols, n_rows = both_ref.shape
    half = n_cols // 2
    chunk = STEP_ROWS
    n_chunks = half // chunk
    me, z = lax.axis_index("arcs"), lax.axis_index("tiles")
    core, chip = lax.rem(me, 2), lax.div(me, 2)
    x, y = lax.rem(chip, 2), lax.div(chip, 2)
    x_peer = me + 2 - 4 * x
    y_peer = me + 4 - 8 * y
    core_peer = me + 1 - 2 * core
    side = lax.div(z, 2)
    step_z = 1 - 2 * side
    inner = (z == 1) | (z == 2)
    outer = jnp.logical_not(inner)
    toward_z = z + step_z
    away_z = jnp.where(inner, z - step_z, z)

    def flip(a, b):
        return a + b - 2 * a * b

    def rows_of(h):
        return pl.ds(pl.multiple_of(h * chunk, chunk), chunk)

    def own_rows(h):
        return pl.ds(pl.multiple_of(core * half + h * chunk, chunk), chunk)

    def remote(src, dst, send, recv, a, zz):
        return pltpu.make_async_remote_copy(
            src_ref=src, dst_ref=dst, send_sem=send, recv_sem=recv,
            device_id=(a, zz), device_id_type=MESH,
        )

    def send_toward(h):
        slot = jnp.where(inner, 0, 1)
        return remote(both_ref.at[own_rows(h)], held_ref.at[slot, rows_of(h)],
                      a_send.at[h], held_recv.at[slot, h], me, toward_z)

    def send_away(h):
        return remote(both_ref.at[own_rows(h)], held_ref.at[0, rows_of(h)],
                      w_send.at[h], held_recv.at[0, h], me, away_z)

    def send_on(h):
        return remote(held_ref.at[1, rows_of(h)], held_ref.at[2, rows_of(h)],
                      b_send.at[h], held_recv.at[2, h], me, toward_z)

    def send_twin(h):
        return remote(held_ref.at[1, rows_of(h)], twin_ref.at[rows_of(h)],
                      twin_send.at[h], twin_recv.at[h], core_peer, z)

    def send_first_twin(away_ref):
        return remote(away_ref, twin_ref.at[rows_of(0)],
                      twin_send.at[0], twin_recv.at[0], core_peer, z)

    def send_first_on(away_ref):
        return remote(away_ref, held_ref.at[2, rows_of(0)],
                      b_send.at[0], held_recv.at[2, 0], me, toward_z)

    def rhs_copy(k):
        return remote(rhs_ref, rhs_in.at[k], rhs_send.at[k], rhs_recv.at[k],
                      lax.rem(me + k + 1, 8), z)

    def arrived(slot, h):
        return remote(held_ref.at[slot, rows_of(h)], held_ref.at[slot, rows_of(h)],
                      a_send.at[h], held_recv.at[slot, h], me, toward_z)

    barrier = pltpu.get_barrier_semaphore()
    for k in range(7):
        pl.semaphore_signal(barrier, inc=1, device_id=(lax.rem(me + k + 1, 8), z),
                            device_id_type=MESH)
    pl.semaphore_signal(barrier, inc=1, device_id=(me, toward_z), device_id_type=MESH)

    @pl.when(inner)
    def _():
        pl.semaphore_signal(barrier, inc=1, device_id=(me, away_z), device_id_type=MESH)
        pl.semaphore_wait(barrier, 9)

    @pl.when(outer)
    def _():
        pl.semaphore_wait(barrier, 8)

    @pl.when(z == 1)
    def _():
        send_first_on(below_ref).start()

    @pl.when(z == 2)
    def _():
        send_first_on(above_ref).start()

    for h in range(1, n_chunks):
        @pl.when(outer | (h < 3))
        def _():
            send_toward(h).start()

        @pl.when(inner)
        def _():
            send_away(h).start()

    for k in range(7):
        rhs_copy(k).start()

    def load(src, dst):
        copy = pltpu.make_async_copy(src, dst, load_sem)
        copy.start()
        copy.wait()

    def weigh_into(kind, first):
        def body(i, carry):
            rows = pl.ds(pl.multiple_of(i * 32, 32), 32)
            value = left[rows, :].astype(jnp.float32) * weight_ref[...]
            at = pl.ds(pl.multiple_of(first + i * 32, 32), 32)
            right[kind, at, :] = value.astype(jnp.bfloat16)
            return carry

        lax.fori_loop(0, chunk // 32, body, 0)

    def stage_own(i):
        rows = rows_of(i)
        return pltpu.make_async_copy(both_ref.at[rows], right.at[1, rows], prep_sem.at[i])

    def prepare_own(i, carry):
        stage_own(i).wait()

        def body(k, carry):
            rows = pl.ds(pl.multiple_of(i * chunk + k * 32, 32), 32)
            value = right[1, rows, :].astype(jnp.float32) * weight_ref[...]
            right[0, rows, :] = value.astype(jnp.bfloat16)
            return carry

        lax.fori_loop(0, chunk // 32, body, 0)
        return carry

    for i in range(2 * n_chunks):
        stage_own(i).start()

    def load_twin(h):
        mine = n_rows // 2
        for src, dst in ((0, mine), (mine, 0)):
            load(twin_ref.at[rows_of(h), pl.ds(src, mine)], left.at[:, pl.ds(dst, mine)])

    def serve_away(h):
        arrived(1, h).wait_recv()
        send_on(h).start()
        send_twin(h).start()

        @pl.when(h == 1)
        def _():
            send_toward(3).start()

        load(held_ref.at[1, rows_of(h)], left)
        weigh_into(1, core * half + h * chunk)
        send_twin(h).wait_recv()
        load_twin(h)
        weigh_into(1, (1 - core) * half + h * chunk)

    def serve_first_away():
        for at, away_ref in ((0, below_ref), (1, above_ref)):
            @pl.when(side == at)
            def _():
                send_first_twin(away_ref).start()
                load(away_ref, left)

        weigh_into(1, core * half)
        send_first_twin(below_ref).wait_recv()
        load_twin(0)
        weigh_into(1, (1 - core) * half)

    lax.fori_loop(0, 2 * n_chunks, prepare_own, 0)

    own, near, back, far = 0, 1, 2, 3
    order = (
        (back, 0, 0), (own, 0, 0), (near, 0, 0), (far, 0, 0), (back, 1, 0), (own, 1, 0),
        (near, 1, 0), (back, 2, 0), (own, 2, 0), (near, 2, 0), (own, 3, 0), (near, 0, 1),
        (far, 0, 1), (near, 1, 1), (far, 1, 0), (far, 1, 1), (back, 3, 0), (near, 2, 1),
        (near, 3, 0), (near, 3, 1), (far, 2, 0), (far, 2, 1), (far, 3, 1), (far, 3, 0),
    )
    steps = len(order)
    first_edge = 11

    def facts(s):
        code = jnp.int32(0)
        for i, (slot, h, edge) in enumerate(order):
            code = code + jnp.where(s == i, slot * 8 + h * 2 + edge, 0)
        slot, h = lax.div(code, 8), lax.rem(lax.div(code, 2), 4)
        is_edge = lax.rem(code, 2) == 1
        ahead = jnp.where(slot == 1, 1, jnp.where(slot == 2, -1, jnp.where(slot == 3, 2, 0)))
        tile = z + step_z * ahead
        plain_near = (slot < 2) & jnp.logical_not(is_edge)
        active = (s >= 0) & (s < steps) & (inner | plain_near)
        tile_x, tile_y = lax.rem(tile + 4, 2), lax.rem(lax.div(tile + 4, 2), 2)
        off_x, off_y = flip(tile_x, x), flip(tile_y, y)
        return h, slot, is_edge, active, off_x, off_y

    low, high = pl.ds(0, half), pl.ds(half, half)

    def far_copy(s, k, h):
        cols = (low, high)[k]
        return remote(sent.at[lax.rem(s, SLOTS), :, cols], far_in.at[k, h],
                      stage_send.at[lax.rem(s, SLOTS), k], far_recv.at[k, h],
                      (x_peer, y_peer)[k], z)

    def near_copy(s, k, h):
        cols = (low, high)[k]
        return remote(sent.at[lax.rem(s, SLOTS), :, cols], near_in.at[k, h],
                      stage_send.at[lax.rem(s, SLOTS), k], near_recv.at[k, h],
                      (x_peer, y_peer)[k], z)

    def last_copy(s, k, h):
        cols = (low, high)[k]
        return remote(joined.at[lax.rem(s, JOINED), :, cols], last_in.at[k, h],
                      join_send.at[lax.rem(s, JOINED), k], last_recv.at[k, h],
                      (y_peer, x_peer)[k], z)

    def edge_copy(s, k, h):
        cols = (low, high)[k]
        return remote(sent.at[lax.rem(s, SLOTS), :, cols], outer_in.at[k, h],
                      stage_send.at[lax.rem(s, SLOTS), k], outer_recv.at[k, h], x_peer, z)

    def sums_copy(s, k, h):
        cols = (low, high)[k]
        return remote(joined.at[lax.rem(s, JOINED), :, cols], sums_ref.at[rows_of(h), (low, high)[k]],
                      join_send.at[lax.rem(s, JOINED), k], sums_recv.at[k, h], me, away_z)

    def relay_copy(k, h):
        return remote(sums_ref.at[rows_of(h), (low, high)[k]], last_sums_ref.at[rows_of(h), (low, high)[k]],
                      relay_send.at[k, h], relay_recv.at[k, h], y_peer, z)

    def out_copy(s, h):
        return pltpu.make_async_copy(
            partial.at[lax.rem(s, SLOTS)], out_ref.at[rows_of(h)], store_sem)

    def compute(s):
        h, slot, is_edge, active, off_x, off_y = facts(s)

        @pl.when(active)
        def _():
            plain = jnp.logical_not(is_edge)

            @pl.when((slot == 1) & plain & (h > 0))
            def _():
                arrived(0, h).wait_recv()

            @pl.when((slot == 2) & (h == 0))
            def _():
                serve_first_away()

            @pl.when((slot == 2) & (h > 0) & (h < 3))
            def _():
                serve_away(h)

            @pl.when(s == first_edge)
            def _():
                serve_away(3)

            @pl.when((slot == 3) & (plain != (h == 3)))
            def _():
                arrived(2, h).wait_recv()

            @pl.when(slot == 0)
            def _():
                load(both_ref.at[own_rows(h)], left)

            @pl.when((slot == 3) | ((slot > 0) & (h > 0)))
            def _():
                load(held_ref.at[jnp.maximum(slot - 1, 0), rows_of(h)], left)

            for at, first_ref in ((2, below_ref), (1, above_ref)):
                @pl.when((h == 0) & (slot == jnp.where(side == 0, at, 3 - at)))
                def _():
                    load(first_ref, left)

            kind = jnp.where(is_edge, 1, 0)
            buf = lax.rem(s, SLOTS)

            def tile_product(n, carry):
                cols = pl.ds(pl.multiple_of(n * 512, 512), 512)
                partial[buf, :, cols] = lax.dot_general(
                    left[...], right[kind, cols, :], (((1,), (1,)), ((), ())),
                    preferred_element_type=jnp.float32,
                )
                return carry

            tiles = n_cols // 512
            lax.fori_loop(0, tiles // 2, tile_product, 0)

            def round_half(cols):
                sent[buf, :, cols] = partial[buf, :, cols].astype(jnp.bfloat16)

            @pl.when(plain & (off_x == 1) & (off_y == 1))
            def _():
                round_half(low)
                far_copy(s, 0, h).start()

            @pl.when(plain & (off_x == 1) & (off_y == 0))
            def _():
                round_half(low)
                near_copy(s, 0, h).start()

            @pl.when(is_edge & (off_x == 1))
            def _():
                round_half(low)
                edge_copy(s, 0, h).start()

            lax.fori_loop(tiles // 2, tiles, tile_product, 0)

            @pl.when(plain & (off_x == 1) & (off_y == 1))
            def _():
                round_half(high)
                far_copy(s, 1, h).start()

            @pl.when(plain & (off_x == 0) & (off_y == 1))
            def _():
                round_half(high)
                near_copy(s, 1, h).start()

            @pl.when(is_edge & (off_x == 1))
            def _():
                round_half(high)
                edge_copy(s, 1, h).start()

    def join(s):
        h, slot, is_edge, active, off_x, off_y = facts(s)
        buf = lax.rem(jnp.maximum(s, 0), SLOTS)
        place = lax.rem(jnp.maximum(s, 0), JOINED)
        plain = jnp.logical_not(is_edge)

        def add(cols, value):
            joined[place, :, cols] = (
                partial[buf, :, cols] + value.astype(jnp.float32)
            ).astype(jnp.bfloat16)

        @pl.when(active & plain & (off_x == 1) & (off_y == 0))
        def _():
            far_copy(s, 1, h).wait_recv()
            add(high, far_in[1, h])
            last_copy(s, 1, h).start()

        @pl.when(active & plain & (off_x == 0) & (off_y == 1))
        def _():
            far_copy(s, 0, h).wait_recv()
            add(low, far_in[0, h])
            last_copy(s, 0, h).start()

        @pl.when(active & is_edge & (off_x == 0))
        def _():
            for k, cols in ((0, low), (1, high)):
                edge_copy(s, k, h).wait_recv()
                add(cols, outer_in[k, h])
                sums_copy(s, k, h).start()

    def finish(s):
        h, slot, is_edge, active, off_x, off_y = facts(s)
        buf = lax.rem(jnp.maximum(s, 0), SLOTS)
        plain = jnp.logical_not(is_edge)

        @pl.when(active & plain & (off_x == 0) & (off_y == 0))
        def _():
            for k, cols in ((0, low), (1, high)):
                near_copy(s, k, h).wait_recv()
                last_copy(s, k, h).wait_recv()
                partial[buf, :, cols] = (
                    partial[buf, :, cols]
                    + near_in[k, h].astype(jnp.float32)
                    + last_in[k, h].astype(jnp.float32)
                )
            out_copy(s, h).start()
            out_copy(s, h).wait()

        @pl.when(active & plain & (off_x == 1) & (off_y == 1))
        def _():
            far_copy(s, 0, h).wait_send()
            far_copy(s, 1, h).wait_send()

        @pl.when(active & plain & (off_x == 1) & (off_y == 0))
        def _():
            near_copy(s, 0, h).wait_send()
            last_copy(s, 1, h).wait_send()

        @pl.when(active & plain & (off_x == 0) & (off_y == 1))
        def _():
            near_copy(s, 1, h).wait_send()
            last_copy(s, 0, h).wait_send()

        @pl.when(active & is_edge & (off_x == 1))
        def _():
            edge_copy(s, 0, h).wait_send()
            edge_copy(s, 1, h).wait_send()

        @pl.when(active & is_edge & (off_x == 0))
        def _():
            sums_copy(s, 0, h).wait_send()
            sums_copy(s, 1, h).wait_send()

    def one_step(s, carry):
        finish(s - LAG_OUT)

        @pl.when(s < steps)
        def _():
            compute(s)

        join(s - LAG_JOIN)
        return carry

    lax.fori_loop(0, steps + LAG_OUT, one_step, 0)

    owner_y = jnp.where(side == 0, 1, 0)

    @pl.when(outer)
    def _():
        for h in range(n_chunks):
            for k in range(2):
                remote(sums_ref.at[rows_of(h), (low, high)[k]], sums_ref.at[rows_of(h), (low, high)[k]],
                       relay_send.at[k, h], sums_recv.at[k, h], me, toward_z).wait_recv()

                @pl.when(y != owner_y)
                def _():
                    relay_copy(k, h).start()

        for h in range(n_chunks):
            for k in range(2):
                @pl.when(y != owner_y)
                def _():
                    relay_copy(k, h).wait_send()

                @pl.when(y == owner_y)
                def _():
                    relay_copy(k, h).wait_recv()

    @pl.when(inner)
    def _():
        send_first_twin(below_ref).wait_send()
        send_first_on(below_ref).wait_send()

    for h in range(1, n_chunks):
        send_toward(h).wait_send()

        @pl.when(inner)
        def _():
            send_away(h).wait_send()
            send_on(h).wait_send()
            send_twin(h).wait_send()

    total = rhs_ref[...]
    for k in range(7):
        rhs_copy(k).wait()
        total = total + rhs_in[k]
    rhs_out_ref[...] = total


def line(design, observations, solution, arc_ids, block_live):
    me, z = lax.axis_index("arcs"), lax.axis_index("tiles")
    core, y = lax.rem(me, 2), lax.div(me, 4)
    rows, columns = design.shape
    half = columns // 2
    chunks = half // STEP_ROWS
    pairs = [(i, i ^ 1) for i in range(8)]

    def in_order(mine, peers):
        return jnp.concatenate([mine, peers], axis=-1)

    turned = design.T
    own_first = lax.dynamic_slice_in_dim(turned, core * half, STEP_ROWS, 0)
    give_first = lax.dynamic_slice_in_dim(turned, (1 - core) * half, STEP_ROWS, 0)
    own_first = in_order(own_first, lax.ppermute(give_first, "arcs", pairs))
    turned, design, own_first = lax.optimization_barrier((turned, design, own_first))
    turned_peer = lax.ppermute(turned, "arcs", pairs)
    row_weight, residual, own_first = row_weights(
        design, observations, solution, arc_ids, block_live, own_first
    )
    below = lax.ppermute(own_first, "tiles", [(0, 1), (1, 2), (2, 3)])
    above = lax.ppermute(own_first, "tiles", [(1, 0), (2, 1), (3, 2)])
    rhs_part = right_side(design, row_weight, residual).reshape(-1, 128)
    weight = in_order(row_weight, lax.ppermute(row_weight, "arcs", pairs))[None, :]
    both = in_order(turned, turned_peer)

    half_dtype, wide = jnp.bfloat16, jnp.float32
    shape = jax.ShapeDtypeStruct
    dma = pltpu.SemaphoreType.DMA
    own, held, twin, sums, last_sums, rhs = pl.pallas_call(
        line_kernel,
        out_shape=(
            shape((half, columns), wide),
            shape((3, half, 2 * rows), half_dtype),
            shape((half, 2 * rows), half_dtype),
            shape((half, columns), half_dtype),
            shape((half, columns), half_dtype),
            shape(rhs_part.shape, wide),
        ),
        in_specs=[
            pl.BlockSpec(memory_space=pl.ANY),
            pl.BlockSpec(memory_space=pltpu.VMEM),
            pl.BlockSpec(memory_space=pltpu.VMEM),
        ]
        + [pl.BlockSpec(memory_space=pl.ANY)] * 2,
        out_specs=[pl.BlockSpec(memory_space=pl.ANY)] * 5
        + [pl.BlockSpec(memory_space=pltpu.VMEM)],
        scratch_shapes=[
            pltpu.VMEM((2, columns, 2 * rows), half_dtype),
            pltpu.VMEM((STEP_ROWS, 2 * rows), half_dtype),
            pltpu.VMEM((7,) + rhs_part.shape, wide),
            pltpu.VMEM((SLOTS, STEP_ROWS, columns), wide),
            pltpu.VMEM((SLOTS, STEP_ROWS, columns), half_dtype),
            pltpu.VMEM((JOINED, STEP_ROWS, columns), half_dtype),
            pltpu.VMEM((2, chunks, STEP_ROWS, half), half_dtype),
            pltpu.VMEM((2, chunks, STEP_ROWS, half), half_dtype),
            pltpu.VMEM((2, chunks, STEP_ROWS, half), half_dtype),
            pltpu.VMEM((2, chunks, STEP_ROWS, half), half_dtype),
            dma, dma, dma((2 * chunks,)),
            dma((chunks,)), dma((chunks,)), dma((chunks,)), dma((chunks,)),
            dma((3, chunks)), dma((chunks,)),
            dma((SLOTS, 2)), dma((JOINED, 2)),
            dma((2, chunks)), dma((2, chunks)), dma((2, chunks)), dma((2, chunks)),
            dma((2, chunks)), dma((2, chunks)), dma((2, chunks)), dma((7,)), dma((7,)),
        ],
        compiler_params=pltpu.CompilerParams(
            collective_id=0, has_side_effects=True, vmem_limit_bytes=67_000_000
        ),
    )(both, weight, rhs_part, below, above)
    edge = sums.astype(wide) + last_sums.astype(wide)
    is_outer_owner = ((z == 0) & (y == 1)) | ((z == 3) & (y == 0))
    normal = jnp.where(is_outer_owner, edge, own)
    return (normal, rhs.reshape(-1))


def solution(mesh):
    n_arcs, n_tiles = mesh.shape["arcs"], mesh.shape["tiles"]

    def local(design, *rest):
        fits = design.shape[1] == 8 * STEP_ROWS and design.shape[1] % 128 == 0
        if n_arcs == 8 and n_tiles == 4 and fits:
            return line(design, *rest)
        return general(design, *rest)

    return jax.shard_map(
        local,
        mesh=mesh,
        in_specs=(P("arcs", "tiles"), P("arcs"), P("tiles"), P("arcs", None), P("arcs", None)),
        out_specs=(P("arcs", "tiles"), P("tiles")),
        check_vma=False,
    )
```
